32 devices in a mesh: row: 8 (over y, x, core), col: 4 (over z).
Axes of the slice: x: 2, y: 2, z: 4, core: 2. Of those that a mesh axis runs over, the one named last changes fastest.
Arguments:
- right_side: float32 [2, 2048, 1024], P(None, 'row', 'col'), may hold values from -6 to 6
- probe: float32 [2, 256, 256], replicated, may hold values from -6 to 6
- detector_weights: float32 [256, 256], replicated, may hold values from 0.1 to 10
- offsets: int32 [8, 4, 4, 2], P('row', 'col'), may hold values from -128 to 127, as said below
- counts: int32 [8, 4], P('row', 'col'), may hold values from 2 to 4, as said below
Outputs:
- solution_field: float32 [2, 2048, 1024], P(None, 'row', 'col')
- residual: float32 [2, 2048, 1024], P(None, 'row', 'col')
The draws below stay inside these ranges and needn't reach their ends.
Inputs may be any that keep to these rules, and one draw needn't show every extreme that they name: `counts`: every region holds at least two positions; in every draw some region holds exactly 4. In every region slot 0 has both offsets negative and slot 1 both offsets non-negative.
All inputs are finite; a program needn't handle non-finite values.
Results may differ from the reference program's by a relative error of at most 0.0003.
Values sent between devices are 32-bit elements; how exact they have to be, the bound alone decides.
No kernel may reach another device: no remote copies, remote signals or barrier semaphores. Data moves between devices by JAX's collectives and lax.ppermute only.
A program may use at most 64 MiB of HBM per device.

```python
import math
import jax
import jax.numpy as jnp
from jax import lax

PATCH = 256
CAP = 4
ITERS = 3
NY = 2048
NX = 1024
N_ROW = 8
N_COL = 4


def draw_counts(key, part):
    key_full, key_low, key_pick = jax.random.split(jax.random.fold_in(key, 71), 3)
    heavy = jax.random.randint(key_full, (N_ROW, N_COL), 0, 4) == 0
    light = jax.random.randint(key_low, (N_ROW, N_COL), 2, max(CAP // 2, 2) + 1)
    filled = jnp.where(heavy, CAP, light).reshape(-1)
    chosen = jax.random.randint(key_pick, (), 0, N_ROW * N_COL)
    filled = filled.at[chosen].set(CAP)
    return filled.reshape(N_ROW, N_COL).astype(jnp.int32)


def draw_offsets(key, part):
    half = PATCH // 2
    key_rest, key_low, key_high = jax.random.split(jax.random.fold_in(key, 53), 3)
    rest = jax.random.randint(key_rest, (N_ROW, N_COL, CAP, 2), -half, half)
    low = jax.random.randint(key_low, (N_ROW, N_COL, 1, 2), -half, 0)
    high = jax.random.randint(key_high, (N_ROW, N_COL, 1, 2), 0, half)
    return jnp.concatenate([low, high, rest[:, :, 2:]], axis=2).astype(jnp.int32)


def shard_levels(stream_key, extent, shards, least, high):
    def one(position, blocks):
        draws = jax.random.uniform(jax.random.fold_in(jax.random.fold_in(stream_key, 6), position), (blocks,), jnp.float32, least / len(shards), high / len(shards))
        return jnp.repeat(jnp.exp(draws), extent[position] // blocks).reshape((-1,) + (1,) * (len(extent) - position - 1))

    gain = one(*shards[0])
    for cut in shards[1:]:
        gain = gain * one(*cut)
    return gain


def centred(own_key, shape, spread, bound, cuts=(), held_as=jnp.bfloat16):
    drawn = jax.random.normal(own_key, shape, jnp.float32) * spread
    if len(cuts) > 0:
        drawn = shard_levels(own_key, shape, cuts, -0.22, 0.18) * drawn
    return jnp.clip(drawn, min=-bound, max=bound).astype(held_as)


def setup_inputs(seed: int = 0) -> dict:
    arg_keys = jax.random.split(jax.random.key(seed), 6)
    return {
        "right_side": centred(arg_keys[0], (2, NY, NX), 1.0, 6.0, ((1, 8), (2, 4)), jnp.float32),
        "probe": centred(arg_keys[1], (2, PATCH, PATCH), 1.0, 6.0, (), jnp.float32),
        "detector_weights": jnp.clip(jnp.exp(jax.random.uniform(arg_keys[2], (PATCH, PATCH), jnp.float32, math.log(0.1), math.log(10.0))), 0.1, 10.0),
        "offsets": draw_offsets(jax.random.fold_in(arg_keys[5], 71), 0),
        "counts": draw_counts(jax.random.fold_in(arg_keys[5], 71), 0),
    }


ridge_weight = 0.5


def patch_normal(tile_in, probe, weights):
    illum = lax.complex(probe[0], probe[1])
    wave = illum * lax.complex(tile_in[0], tile_in[1])
    freq = jnp.fft.fft2(wave, norm="ortho")
    back = jnp.fft.ifft2(freq * weights, norm="ortho")
    result = jnp.conj(illum) * back
    return jnp.stack([jnp.real(result), jnp.imag(result)])


def operate(field, probe, weights, row_starts, col_starts, weight_on):
    margin = PATCH // 2
    padded = jnp.pad(field, ((0, 0), (margin, margin), (margin, margin)))

    def visit(summed, item):
        row_at, col_at, flag = item
        zero_idx = jnp.zeros((), jnp.int32)
        tile_in = lax.dynamic_slice(padded, (zero_idx, row_at, col_at), (2, PATCH, PATCH))
        update = patch_normal(tile_in, probe, weights) * flag
        current = lax.dynamic_slice(summed, (zero_idx, row_at, col_at), (2, PATCH, PATCH))
        return lax.dynamic_update_slice(summed, current + update, (zero_idx, row_at, col_at)), None

    summed, _ = lax.scan(visit, jnp.zeros_like(padded), (row_starts, col_starts, weight_on))
    return summed[:, margin:margin + NY, margin:margin + NX] + ridge_weight * field


def inner(first, second):
    return jnp.sum(first * second)


def reference(right_side, probe, detector_weights, offsets, counts):
    margin = PATCH // 2
    region_row = (jnp.arange(N_ROW, dtype=jnp.int32) * PATCH + margin)[:, None, None]
    region_col = (jnp.arange(N_COL, dtype=jnp.int32) * PATCH + margin)[None, :, None]
    row_starts = (offsets[:, :, :, 0].astype(jnp.int32) + region_row).reshape(-1).astype(jnp.int32)
    col_starts = (offsets[:, :, :, 1].astype(jnp.int32) + region_col).reshape(-1).astype(jnp.int32)
    slot_ids = jnp.arange(CAP, dtype=jnp.int32)[None, None, :]
    weight_on = (slot_ids < counts[:, :, None]).astype(jnp.float32).reshape(-1)
    solution_field = jnp.zeros_like(right_side)
    residual, direction = right_side, right_side
    norm_now = inner(residual, residual)
    for iteration in range(ITERS):
        image = operate(direction, probe, detector_weights, row_starts, col_starts, weight_on)
        alpha = norm_now / inner(direction, image)
        solution_field = solution_field + alpha * direction
        residual = residual - alpha * image
        norm_next = inner(residual, residual)
        direction = residual + (norm_next / norm_now) * direction
        norm_now = norm_next
    return solution_field, residual
```

```python
import functools
import math

import jax
import jax.numpy as jnp
import numpy as np
from jax import lax
from jax.experimental import pallas as pl
from jax.experimental.pallas import tpu as pltpu
from jax.sharding import PartitionSpec as P

ITERS = 3
RIDGE = 0.5
CHUNK = 16
F32 = jnp.float32
BF16 = jnp.bfloat16
VMEM = pl.BlockSpec(memory_space=pltpu.VMEM)
SMEM = pl.BlockSpec(memory_space=pltpu.SMEM)


def pairs(axis, parity):
    count = lax.axis_size(axis)
    out = []
    for low in range(parity, count - 1, 2):
        out += [(low, low + 1), (low + 1, low)]
    return out


def swap(value, axis, parity):
    return lax.ppermute(value, axis, pairs(axis, parity))


def all_sum(value):
    for axis in ("row", "col"):
        count = lax.axis_size(axis)
        if count & (count - 1):
            value = lax.psum(value, axis)
            continue
        step = 1
        while step < count:
            value = value + lax.ppermute(value, axis, [(i, i ^ step) for i in range(count)])
            step *= 2
    return value


def split_np(mat):
    high = mat.astype(np.float32).astype(jnp.bfloat16)
    low = (mat - high.astype(np.float64)).astype(np.float32).astype(jnp.bfloat16)
    return high, low


def tables(length):
    half = length // 2
    spot = np.arange(half)
    lanes, rows = [], []
    for odd in (0, 1):
        phase = (spot[:, None] * (2 * spot[None, :] + odd)) % length
        angle = phase * (2.0 * math.pi / length)
        cos = np.cos(angle) / math.sqrt(length)
        sin = np.sin(angle) / math.sqrt(length)
        forward = np.block([[cos, -sin], [sin, cos]])
        for mat in (forward, forward.T):
            high, low = split_np(mat)
            lanes.append(np.concatenate([high, high, low], axis=0))
            high, low = split_np(mat.T)
            rows.append(np.concatenate([high, low, high], axis=1))
    return np.stack(lanes), np.stack(rows)


def split(value):
    high = value.astype(BF16)
    low = (value - high.astype(F32)).astype(BF16)
    return high, low


def dot(left, right):
    return jnp.dot(left, right, preferred_element_type=F32)


def total(ref):
    return jnp.sum(ref, keepdims=True)


def prep_kernel(side, cap, info, block, probe, zone_a, zone_b, rolled):
    half = side // 2
    par_r, par_c = info[0], info[1]
    for cz, out in ((0, zone_a), (1, zone_b)):
        right = (cz ^ 1 ^ par_c) == 1
        for rz in (0, 1):
            base = pl.multiple_of((rz ^ 1 ^ par_r) * half, half)
            for comp in (0, 1):
                rows = block[comp, pl.ds(base, half), :]
                out[rz, comp] = jnp.where(right, rows[:, half:], rows[:, :half])

    for slot in range(cap):
        row_by = lax.rem(info[5 + 2 * slot] + side, side)
        col_by = lax.rem(info[6 + 2 * slot] + side, side)
        for comp in (0, 1):
            moved = pltpu.roll(probe[comp], row_by, 0)
            rolled[slot, comp] = pltpu.roll(moved, col_by, 1)


def coefficients(stage, sums):
    norms = [total(s[0]) for s in sums]
    prods = [total(s[1]) for s in sums]
    alphas, ratios = [], []
    for k in range(stage):
        if k == 0:
            alphas.append(norms[0] / prods[0])
            ratios.append(None)
        else:
            ratio = norms[k] / norms[k - 1]
            ratios.append(ratio)
            alphas.append(norms[k] / (prods[k] - ratio * norms[k] / alphas[k - 1]))
    return alphas, ratios


def apply_kernel(side, cap, stage, *refs):
    half = side // 2
    n_sums = stage
    info, rolled, weights, lanes, rows = refs[:5]
    pos = 5
    sums = refs[pos : pos + n_sums]
    pos += n_sums
    window = refs[pos : pos + 4]
    pos += 4
    if stage >= 1:
        field_old = refs[pos]
        pos += 1
    if stage >= 2:
        along_old = refs[pos]
        pos += 1
    field = refs[pos]
    pos += 1
    if stage >= 1:
        along = refs[pos]
        pos += 1
    own_out = refs[pos : pos + 2]
    far_out = refs[pos + 2 : pos + 4]
    partial = refs[pos + 4]
    pos += 5
    lhs, mid, rhs, freq, terms = refs[pos : pos + 5]

    par_r, par_c, count = info[0], info[1], info[4]

    if stage == 0:
        for z in range(4):
            for b in range(8):
                idx = (b // 4, (b // 2) % 2, b % 2)
                field[(z,) + idx] = window[z][idx]
    else:
        alphas, ratios = coefficients(stage, sums)
        alpha, ratio = alphas[-1], ratios[-1]
        for z in range(4):
            for b in range(8):
                idx = (b // 4, (b // 2) % 2, b % 2)
                for q in range(0, half, 2 * CHUNK):
                    at = (z,) + idx + (slice(q, q + 2 * CHUNK),)
                    value = window[z][idx + (slice(q, q + 2 * CHUNK),)]
                    if stage >= 2:
                        value = value + ratio * along_old[at]
                    along[at] = value
                    field[at] = field_old[at] - alpha * value

    partial[...] = jnp.zeros_like(partial)

    @pl.when(count <= 2)
    def _():
        terms[2:] = jnp.zeros_like(terms[2:])

    row_iota = lax.broadcasted_iota(jnp.int32, (CHUNK, half), 0)
    col_iota = lax.broadcasted_iota(jnp.int32, (CHUNK, half), 1)

    def marks(slot):
        out = []
        for d in (0, 1):
            off = info[5 + 2 * slot + d]
            neg = off < 0
            out.append(jnp.where(neg, -1, 1))
            out.append(jnp.where(neg, 1 - (off + side), off))
        return out

    def visit(pair, carry):
        slots = (2 * pair, 2 * pair + 1)
        for j, slot in enumerate(slots):
            row_sign, row_from, col_sign, col_from = marks(slot)
            col_own = [(col_iota + l * half) * col_sign >= col_from for l in (0, 1)]
            for h in (0, 1):
                own_z = h ^ 1 ^ par_r
                far_z = 2 + (h ^ par_r)
                for q in range(0, half, CHUNK):
                    row_own = (row_iota + (h * half + q)) * row_sign >= row_from
                    cut = slice(q, q + CHUNK)
                    waves = []
                    for l in (0, 1):
                        own_c = l ^ 1 ^ par_c
                        far_c = l ^ par_c
                        got = []
                        for comp in (0, 1):
                            near = jnp.where(
                                col_own[l],
                                field[own_z, own_c, 0, comp, cut],
                                field[own_z, far_c, 1, comp, cut],
                            )
                            beyond = jnp.where(
                                col_own[l],
                                field[far_z, own_c, 0, comp, cut],
                                field[far_z, far_c, 1, comp, cut],
                            )
                            got.append(jnp.where(row_own, near, beyond))
                        at = (slice(h * half + q, h * half + q + CHUNK), slice(l * half, l * half + half))
                        p_re = rolled[(slot, 0) + at]
                        p_im = rolled[(slot, 1) + at]
                        waves.append((p_re * got[0] - p_im * got[1], p_re * got[1] + p_im * got[0]))
                    to = slice(j * side + h * half + q, j * side + h * half + q + CHUNK)
                    for comp in (0, 1):
                        a, b = waves[0][comp], waves[1][comp]
                        for odd, value in ((0, a + b), (1, a - b)):
                            high, low = split(value)
                            lo_at = comp * half
                            lhs[odd, to, lo_at : lo_at + half] = high
                            lhs[odd, to, side + lo_at : side + lo_at + half] = low
                            lhs[odd, to, 2 * side + lo_at : 2 * side + lo_at + half] = high

        for odd in (0, 1):
            mid[odd] = dot(lhs[odd], lanes[2 * odd])

        for j in (0, 1):
            for odd in (0, 1):
                for q in range(0, half, CHUNK):
                    top = mid[odd, j * side + q : j * side + q + CHUNK]
                    low_rows = mid[odd, j * side + half + q : j * side + half + q + CHUNK]
                    for which, value in ((0, top + low_rows), (1, top - low_rows)):
                        for comp in (0, 1):
                            high, low = split(value[:, comp * half : comp * half + half])
                            to = slice(j * side + odd * half, j * side + odd * half + half)
                            k = comp * half + q
                            rhs[which, k : k + CHUNK, to] = high
                            rhs[which, side + k : side + k + CHUNK, to] = high
                            rhs[which, 2 * side + k : 2 * side + k + CHUNK, to] = low

        for which in (0, 1):
            freq[which] = dot(rows[2 * which], rhs[which])

        for which in (0, 1):
            gathered = [jnp.zeros((8, half), F32), jnp.zeros((8, half), F32)]
            for j in (0, 1):
                for odd in (0, 1):
                    to = slice(j * side + odd * half, j * side + odd * half + half)
                    for comp in (0, 1):
                        for q in range(0, half, CHUNK):
                            value = freq[which, comp * half + q : comp * half + q + CHUNK, to]
                            scaled = value * weights[which, q : q + CHUNK, odd * half : odd * half + half]
                            both = value * scaled
                            for e in range(0, CHUNK, 8):
                                gathered[j] = gathered[j] + both[e : e + 8]
                            high, low = split(scaled)
                            k = comp * half + q
                            rhs[which, k : k + CHUNK, to] = high
                            rhs[which, side + k : side + k + CHUNK, to] = high
                            rhs[which, 2 * side + k : 2 * side + k + CHUNK, to] = low
            for j, slot in enumerate(slots):
                partial[1] += jnp.where(slot < count, gathered[j], 0.0)

        for which in (0, 1):
            freq[which] = dot(rows[2 * which + 1], rhs[which])

        for j in (0, 1):
            for odd in (0, 1):
                to = slice(j * side + odd * half, j * side + odd * half + half)
                for comp in (0, 1):
                    for q in range(0, half, CHUNK):
                        even_part = freq[0, comp * half + q : comp * half + q + CHUNK, to]
                        odd_part = freq[1, comp * half + q : comp * half + q + CHUNK, to]
                        for h, value in ((0, even_part + odd_part), (1, even_part - odd_part)):
                            high, low = split(value)
                            at = slice(j * side + h * half + q, j * side + h * half + q + CHUNK)
                            lo_at = comp * half
                            lhs[odd, at, lo_at : lo_at + half] = high
                            lhs[odd, at, side + lo_at : side + lo_at + half] = low
                            lhs[odd, at, 2 * side + lo_at : 2 * side + lo_at + half] = high

        for odd in (0, 1):
            mid[odd] = dot(lhs[odd], lanes[2 * odd + 1])

        for j, slot in enumerate(slots):
            used = slot < count
            for h in (0, 1):
                for q in range(0, half, CHUNK):
                    at = slice(j * side + h * half + q, j * side + h * half + q + CHUNK)
                    even_part, odd_part = mid[0, at], mid[1, at]
                    for l, value in ((0, even_part + odd_part), (1, even_part - odd_part)):
                        v_re, v_im = value[:, :half], value[:, half:]
                        spot = (slice(h * half + q, h * half + q + CHUNK), slice(l * half, l * half + half))
                        p_re = rolled[(slot, 0) + spot]
                        p_im = rolled[(slot, 1) + spot]
                        cut = slice(q, q + CHUNK)
                        terms[slot, h, l, 0, cut] = jnp.where(used, p_re * v_re + p_im * v_im, 0.0)
                        terms[slot, h, l, 1, cut] = jnp.where(used, p_re * v_im - p_im * v_re, 0.0)
        return carry

    lax.fori_loop(0, (count + 1) // 2, visit, 0)

    norm = jnp.zeros((8, half), F32)
    for rz in (0, 1):
        for rk, out in ((0, own_out[rz]), (1, far_out[rz])):
            h = (rz ^ par_r) if rk else (rz ^ 1 ^ par_r)
            for cz in (0, 1):
                for ck in (0, 1):
                    l = (cz ^ par_c) if ck else (cz ^ 1 ^ par_c)
                    col_masks, row_marks = [], []
                    for slot in range(cap):
                        row_sign, row_from, col_sign, col_from = marks(slot)
                        own = (col_iota + l * half) * col_sign >= col_from
                        col_masks.append(jnp.logical_not(own) if ck else own)
                        row_marks.append((row_sign, row_from))
                    for q in range(0, half, CHUNK):
                        cut = slice(q, q + CHUNK)
                        acc = [None, None]
                        if rk == 0 and ck == 0:
                            for comp in (0, 1):
                                value = field[rz, cz, 0, comp, cut]
                                acc[comp] = RIDGE * value
                                sq = value * value
                                for e in range(0, CHUNK, 8):
                                    norm = norm + sq[e : e + 8]
                        for slot in range(cap):
                            row_sign, row_from = row_marks[slot]
                            spots = (row_iota + (h * half + q)) * row_sign
                            mask = (spots < row_from) if rk else (spots >= row_from)
                            mask = jnp.logical_and(mask, col_masks[slot])
                            for comp in (0, 1):
                                value = jnp.where(mask, terms[slot, h, l, comp, cut], 0.0)
                                acc[comp] = value if acc[comp] is None else acc[comp] + value
                        for comp in (0, 1):
                            out[cz, ck, comp, cut] = acc[comp]
    partial[0] = norm
    partial[1] += RIDGE * norm


def final_kernel(side, stage, *refs):
    half = side // 2
    info = refs[0]
    sums = refs[1 : 1 + stage]
    fields = refs[1 + stage : 1 + 2 * stage]
    along_old = refs[1 + 2 * stage]
    mine = refs[2 + 2 * stage : 6 + 2 * stage]
    theirs = refs[6 + 2 * stage : 10 + 2 * stage]
    solved, left = refs[10 + 2 * stage :]
    par_r, par_c = info[0], info[1]
    alphas, ratios = coefficients(stage, sums)
    for rz in (0, 1):
        for cz in (0, 1):
            for comp in (0, 1):
                for q in range(0, half, 2 * CHUNK):
                    cut = slice(q, q + 2 * CHUNK)
                    image = mine[2 * rz + cz][0, comp, cut] + theirs[2 * rz + cz][comp, cut]
                    value = image + ratios[-1] * along_old[rz, cz, 0, comp, cut]
                    residual = fields[-1][rz, cz, 0, comp, cut]
                    direction = fields[0][rz, cz, 0, comp, cut]
                    answer = alphas[0] * direction
                    for k in range(1, stage):
                        direction = fields[k][rz, cz, 0, comp, cut] + ratios[k] * direction
                        answer = answer + alphas[k] * direction
                    residual = residual - alphas[-1] * value
                    at = pl.ds(pl.multiple_of((rz ^ 1 ^ par_r) * half + q, 2 * CHUNK), 2 * CHUNK)
                    for right in (0, 1):
                        @pl.when((cz ^ 1 ^ par_c) == right)
                        def _():
                            solved[comp, at, right * half : right * half + half] = answer
                            left[comp, at, right * half : right * half + half] = residual


def local(right_side, probe, detector_weights, offsets, counts):
    side = probe.shape[1]
    half = side // 2
    cap = offsets.shape[2]
    row_at, col_at = lax.axis_index("row"), lax.axis_index("col")
    row_n, col_n = lax.axis_size("row"), lax.axis_size("col")
    par_r, par_c = row_at % 2, col_at % 2

    def partner(at, par, count, zone):
        other = at + (1 - 2 * (par ^ zone))
        return jnp.logical_and(other >= 0, other < count)

    near_col = [partner(col_at, par_c, col_n, z).astype(F32) for z in (0, 1)]
    info = jnp.concatenate(
        [
            jnp.stack([par_r, par_c, par_r, par_c, counts[0, 0]]).astype(jnp.int32),
            offsets.reshape(-1).astype(jnp.int32),
        ]
    )
    lanes, rows = tables(side)
    lanes, rows = jnp.asarray(lanes), jnp.asarray(rows)
    weights = (
        detector_weights.reshape(half, 2, half, 2).transpose(1, 0, 3, 2).reshape(2, half, side)
    )

    zone = jax.ShapeDtypeStruct((2, 2, half, half), F32)
    strip = jax.ShapeDtypeStruct((2, 2, 2, half, half), F32)
    whole = jax.ShapeDtypeStruct((4, 2, 2, 2, half, half), F32)
    tiny = jax.ShapeDtypeStruct((2, 8, half), F32)

    zone_a, zone_b, rolled = pl.pallas_call(
        functools.partial(prep_kernel, side, cap),
        out_shape=(zone, zone, jax.ShapeDtypeStruct((cap, 2, side, side), F32)),
        in_specs=[SMEM, VMEM, VMEM],
        out_specs=(VMEM, VMEM, VMEM),
        compiler_params=pltpu.CompilerParams(vmem_limit_bytes=16 * 2**20),
    )(info, right_side, probe)

    def apply_op(stage, sums, window, field_old, along_old):
        args = [info, rolled, weights, lanes, rows, *sums, *window]
        outs = [whole]
        if stage >= 1:
            args.append(field_old)
            outs.append(whole)
        if stage >= 2:
            args.append(along_old)
        outs += [strip] * 4 + [tiny]
        got = pl.pallas_call(
            functools.partial(apply_kernel, side, cap, stage),
            out_shape=tuple(outs),
            in_specs=[SMEM] + [VMEM] * (len(args) - 1),
            out_specs=tuple([VMEM] * len(outs)),
            scratch_shapes=[
                pltpu.VMEM((2, 2 * side, 3 * side), BF16),
                pltpu.VMEM((2, 2 * side, side), F32),
                pltpu.VMEM((2, 3 * side, 2 * side), BF16),
                pltpu.VMEM((2, side, 2 * side), F32),
                pltpu.VMEM((cap, 2, 2, 2, half, half), F32),
            ],
            compiler_params=pltpu.CompilerParams(vmem_limit_bytes=32 * 2**20),
        )(*args)
        field = got[0]
        along = got[1] if stage >= 1 else None
        rest = got[2:] if stage >= 1 else got[1:]
        return field, along, rest[0:2], rest[2:4], rest[4]

    zones = (zone_a, zone_b)
    beyond = [swap(zones[z], "col", z) for z in (0, 1)]
    near = [
        jnp.stack([jnp.stack([zones[cz][rz], beyond[cz][rz]]) for cz in (0, 1)]) for rz in (0, 1)
    ]
    far = [swap(near[z], "row", z) for z in (0, 1)]
    window = (near[0], near[1], far[0], far[1])

    sums, fields = [], []
    field = along = None
    for stage in range(ITERS):
        field, along_new, own, sent, partial = apply_op(stage, sums, window, field, along)
        fields.append(field)
        along = along_new
        reduced = [own[z] + swap(sent[z], "row", z) for z in (0, 1)]
        sums = sums + [all_sum(partial)]
        mine = [reduced[rz][cz] for rz in (0, 1) for cz in (0, 1)]
        if stage + 1 < ITERS:
            got = [swap(mine[2 * rz + cz], "col", cz) for rz in (0, 1) for cz in (0, 1)]
            near = []
            for rz in (0, 1):
                parts = []
                for cz in (0, 1):
                    m, g = mine[2 * rz + cz], got[2 * rz + cz]
                    parts.append(jnp.stack([m[0] + g[1], (m[1] + g[0]) * near_col[cz]]))
                near.append(jnp.stack(parts))
            far = [swap(near[z], "row", z) for z in (0, 1)]
            window = (near[0], near[1], far[0], far[1])
        else:
            got = [swap(mine[2 * rz + cz][1], "col", cz) for rz in (0, 1) for cz in (0, 1)]

    out = jax.ShapeDtypeStruct(right_side.shape, F32)
    args = [info, *sums, *fields, along, *mine, *got]
    return pl.pallas_call(
        functools.partial(final_kernel, side, ITERS),
        out_shape=(out, out),
        in_specs=[SMEM] + [VMEM] * (len(args) - 1),
        out_specs=(VMEM, VMEM),
        compiler_params=pltpu.CompilerParams(vmem_limit_bytes=16 * 2**20),
    )(*args)


def solution(mesh):
    placed = (P(None, "row", "col"), P(), P(), P("row", "col", None, None), P("row", "col"))
    return jax.shard_map(
        local,
        mesh=mesh,
        in_specs=placed,
        out_specs=(P(None, "row", "col"), P(None, "row", "col")),
        check_vma=False,
    )
```

```python
import functools
import math

import jax
import jax.numpy as jnp
import numpy as np
from jax import lax
from jax.experimental import pallas as pl
from jax.experimental.pallas import tpu as pltpu
from jax.sharding import PartitionSpec as P

ITERS = 3
RIDGE = 0.5
CHUNK = 16
F32 = jnp.float32
BF16 = jnp.bfloat16
VMEM = pl.BlockSpec(memory_space=pltpu.VMEM)
SMEM = pl.BlockSpec(memory_space=pltpu.SMEM)


def pairs(axis, parity):
    count = lax.axis_size(axis)
    out = []
    for low in range(parity, count - 1, 2):
        out += [(low, low + 1), (low + 1, low)]
    return out


def swap(value, axis, parity):
    return lax.ppermute(value, axis, pairs(axis, parity))


def split_np(mat):
    high = mat.astype(np.float32).astype(jnp.bfloat16)
    low = (mat - high.astype(np.float64)).astype(np.float32).astype(jnp.bfloat16)
    return high, low


def tables(length):
    half = length // 2
    spot = np.arange(half)
    out = []
    for odd in (0, 1):
        phase = (spot[:, None] * (2 * spot[None, :] + odd)) % length
        angle = phase * (2.0 * math.pi / length)
        cos = np.cos(angle) / math.sqrt(length)
        sin = np.sin(angle) / math.sqrt(length)
        forward = np.block([[cos, -sin], [sin, cos]])
        for mat in (forward, forward.T):
            out.append(np.stack(split_np(mat)))
    return np.stack(out)


def split(value):
    high = value.astype(BF16)
    low = (value - high.astype(F32)).astype(BF16)
    return high, low


def dot(left, right):
    return jnp.dot(left, right, preferred_element_type=F32)


def total(ref):
    return jnp.sum(ref, keepdims=True)


def parities():
    return lax.axis_index("row") % 2, lax.axis_index("col") % 2


def zone_kernel(side, block, zone_a, zone_b):
    half = side // 2
    par_r, par_c = parities()
    for cz, out in ((0, zone_a), (1, zone_b)):
        right = (cz ^ 1 ^ par_c) == 1
        for rz in (0, 1):
            base = pl.multiple_of((rz ^ 1 ^ par_r) * half, half)
            for comp in (0, 1):
                rows = block[comp, pl.ds(base, half), :]
                out[rz, comp] = jnp.where(right, rows[:, half:], rows[:, :half])


def prep_kernel(side, cap, info, probe, weights, mats, rolled, sorted_weights, lanes, rows, held):
    half = side // 2
    for f in range(4):
        high, low = mats[f, 0], mats[f, 1]
        lanes[f, :side] = high
        lanes[f, side : 2 * side] = high
        lanes[f, 2 * side :] = low
        other = f ^ 1
        rows[other, :, :side] = high
        rows[other, :, side : 2 * side] = low
        rows[other, :, 2 * side :] = high

    source = lax.broadcasted_iota(jnp.int32, (side, side), 0)
    target = lax.broadcasted_iota(jnp.int32, (side, side), 1)
    wanted = jnp.where(target < half, 2 * target, 2 * (target - half) + 1)
    pick = jnp.where(source == wanted, 1.0, 0.0).astype(BF16)
    value = weights[...]
    first = value.astype(BF16)
    rest = value - first.astype(F32)
    second = rest.astype(BF16)
    third = (rest - second.astype(F32)).astype(BF16)
    moved = (dot(first, pick) + dot(second, pick)) + dot(third, pick)
    for odd in (0, 1):
        held[odd] = moved[:, odd * half : odd * half + half]
    for which in (0, 1):
        for odd in (0, 1):
            to = slice(odd * half, odd * half + half)
            sorted_weights[which, :, to] = held[odd, pl.ds(which, half, stride=2), :]

    for slot in range(cap):
        row_by = lax.rem(info[1 + 2 * slot] + side, side)
        col_by = lax.rem(info[2 + 2 * slot] + side, side)
        for comp in (0, 1):
            turned = pltpu.roll(probe[comp], row_by, 0)
            rolled[slot, comp] = pltpu.roll(turned, col_by, 1)


def reduce_kernel(own, got, sum_a, sum_b, out_a, out_b, sum_out):
    for cz, out in ((0, out_a), (1, out_b)):
        for b in range(4):
            out[b // 2, b % 2] = own[cz, b // 2, b % 2] + got[cz, b // 2, b % 2]
    sum_out[...] = sum_a[...] + sum_b[...]


def has_partner(axis, zone):
    at, count = lax.axis_index(axis), lax.axis_size(axis)
    other = at + 1 - 2 * ((at % 2) ^ zone)
    return jnp.logical_and(other >= 0, other < count)


def merge_kernel(mine_a, mine_b, got_a, got_b, sum_a, sum_b, out, sum_out):
    for cz, mine, got in ((0, mine_a, got_a), (1, mine_b, got_b)):
        inside = has_partner("col", cz)
        for comp in (0, 1):
            out[cz, 0, comp] = mine[0, comp] + got[1, comp]
            out[cz, 1, comp] = jnp.where(inside, mine[1, comp] + got[0, comp], 0.0)
    sum_out[...] = sum_a[...] + sum_b[...]


def first_kernel(zone_a, zone_b, got_a, got_b, out_a, out_b):
    for cz, zone, got in ((0, zone_a, got_a), (1, zone_b, got_b)):
        for rz, out in ((0, out_a), (1, out_b)):
            for comp in (0, 1):
                out[cz, 0, comp] = zone[rz, comp]
                out[cz, 1, comp] = got[rz, comp]


def add_kernel(sum_a, sum_b, sum_out):
    sum_out[...] = sum_a[...] + sum_b[...]


def coefficients(stage, sums):
    norms = [total(a[0] + b[0]) for a, b in zip(sums[::2], sums[1::2])]
    prods = [total(a[1] + b[1]) for a, b in zip(sums[::2], sums[1::2])]
    alphas, ratios = [], []
    for k in range(stage):
        if k == 0:
            alphas.append(norms[0] / prods[0])
            ratios.append(None)
        else:
            ratio = norms[k] / norms[k - 1]
            ratios.append(ratio)
            alphas.append(norms[k] / (prods[k] - ratio * norms[k] / alphas[k - 1]))
    return alphas, ratios


def apply_kernel(side, cap, stage, *refs):
    half = side // 2
    n_sums = 2 * stage
    info, rolled, weights, lanes, rows = refs[:5]
    pos = 5
    sums = refs[pos : pos + n_sums]
    pos += n_sums
    window = refs[pos : pos + 4]
    pos += 4
    if stage >= 1:
        field_old = refs[pos]
        pos += 1
    if stage >= 2:
        along_old = refs[pos]
        pos += 1
    field = refs[pos]
    pos += 1
    if stage >= 1:
        along = refs[pos]
        pos += 1
    own_out = refs[pos : pos + 2]
    far_out = refs[pos + 2 : pos + 4]
    partial = refs[pos + 4]
    pos += 5
    lhs, mid, rhs, freq, terms = refs[pos : pos + 5]

    par_r, par_c = parities()
    count = info[0]

    if stage == 0:
        for z in range(4):
            for b in range(8):
                idx = (b // 4, (b // 2) % 2, b % 2)
                field[(z,) + idx] = window[z][idx]
    else:
        alphas, ratios = coefficients(stage, sums)
        alpha, ratio = alphas[-1], ratios[-1]
        for z in range(4):
            for b in range(8):
                idx = (b // 4, (b // 2) % 2, b % 2)
                for q in range(0, half, 2 * CHUNK):
                    at = (z,) + idx + (slice(q, q + 2 * CHUNK),)
                    value = window[z][idx + (slice(q, q + 2 * CHUNK),)]
                    if stage >= 2:
                        value = value + ratio * along_old[at]
                    along[at] = value
                    field[at] = field_old[at] - alpha * value

    partial[...] = jnp.zeros_like(partial)

    @pl.when(count <= 2)
    def _():
        terms[2:] = jnp.zeros_like(terms[2:])

    row_iota = lax.broadcasted_iota(jnp.int32, (CHUNK, half), 0)
    col_iota = lax.broadcasted_iota(jnp.int32, (CHUNK, half), 1)

    def marks(slot):
        out = []
        for d in (0, 1):
            off = info[1 + 2 * slot + d]
            neg = off < 0
            out.append(jnp.where(neg, -1, 1))
            out.append(jnp.where(neg, 1 - (off + side), off))
        return out

    def visit(pair, carry):
        slots = (2 * pair, 2 * pair + 1)
        for j, slot in enumerate(slots):
            row_sign, row_from, col_sign, col_from = marks(slot)
            col_own = [(col_iota + l * half) * col_sign >= col_from for l in (0, 1)]
            for h in (0, 1):
                own_z = h ^ 1 ^ par_r
                far_z = 2 + (h ^ par_r)
                for q in range(0, half, CHUNK):
                    row_own = (row_iota + (h * half + q)) * row_sign >= row_from
                    cut = slice(q, q + CHUNK)
                    waves = []
                    for l in (0, 1):
                        own_c = l ^ 1 ^ par_c
                        far_c = l ^ par_c
                        got = []
                        for comp in (0, 1):
                            near = jnp.where(
                                col_own[l],
                                field[own_z, own_c, 0, comp, cut],
                                field[own_z, far_c, 1, comp, cut],
                            )
                            beyond = jnp.where(
                                col_own[l],
                                field[far_z, own_c, 0, comp, cut],
                                field[far_z, far_c, 1, comp, cut],
                            )
                            got.append(jnp.where(row_own, near, beyond))
                        at = (slice(h * half + q, h * half + q + CHUNK), slice(l * half, l * half + half))
                        p_re = rolled[(slot, 0) + at]
                        p_im = rolled[(slot, 1) + at]
                        waves.append((p_re * got[0] - p_im * got[1], p_re * got[1] + p_im * got[0]))
                    to = slice(j * side + h * half + q, j * side + h * half + q + CHUNK)
                    for comp in (0, 1):
                        a, b = waves[0][comp], waves[1][comp]
                        for odd, value in ((0, a + b), (1, a - b)):
                            high, low = split(value)
                            lo_at = comp * half
                            lhs[odd, to, lo_at : lo_at + half] = high
                            lhs[odd, to, side + lo_at : side + lo_at + half] = low
                            lhs[odd, to, 2 * side + lo_at : 2 * side + lo_at + half] = high

        for odd in (0, 1):
            mid[odd] = dot(lhs[odd], lanes[2 * odd])

        for j in (0, 1):
            for odd in (0, 1):
                for q in range(0, half, CHUNK):
                    top = mid[odd, j * side + q : j * side + q + CHUNK]
                    low_rows = mid[odd, j * side + half + q : j * side + half + q + CHUNK]
                    for which, value in ((0, top + low_rows), (1, top - low_rows)):
                        for comp in (0, 1):
                            high, low = split(value[:, comp * half : comp * half + half])
                            to = slice(j * side + odd * half, j * side + odd * half + half)
                            k = comp * half + q
                            rhs[which, k : k + CHUNK, to] = high
                            rhs[which, side + k : side + k + CHUNK, to] = high
                            rhs[which, 2 * side + k : 2 * side + k + CHUNK, to] = low

        for which in (0, 1):
            freq[which] = dot(rows[2 * which], rhs[which])

        for which in (0, 1):
            gathered = [jnp.zeros((8, half), F32), jnp.zeros((8, half), F32)]
            for j in (0, 1):
                for odd in (0, 1):
                    to = slice(j * side + odd * half, j * side + odd * half + half)
                    for comp in (0, 1):
                        for q in range(0, half, CHUNK):
                            value = freq[which, comp * half + q : comp * half + q + CHUNK, to]
                            scaled = value * weights[which, q : q + CHUNK, odd * half : odd * half + half]
                            both = value * scaled
                            for e in range(0, CHUNK, 8):
                                gathered[j] = gathered[j] + both[e : e + 8]
                            high, low = split(scaled)
                            k = comp * half + q
                            rhs[which, k : k + CHUNK, to] = high
                            rhs[which, side + k : side + k + CHUNK, to] = high
                            rhs[which, 2 * side + k : 2 * side + k + CHUNK, to] = low
            for j, slot in enumerate(slots):
                partial[1] += jnp.where(slot < count, gathered[j], 0.0)

        for which in (0, 1):
            freq[which] = dot(rows[2 * which + 1], rhs[which])

        for j in (0, 1):
            for odd in (0, 1):
                to = slice(j * side + odd * half, j * side + odd * half + half)
                for comp in (0, 1):
                    for q in range(0, half, CHUNK):
                        even_part = freq[0, comp * half + q : comp * half + q + CHUNK, to]
                        odd_part = freq[1, comp * half + q : comp * half + q + CHUNK, to]
                        for h, value in ((0, even_part + odd_part), (1, even_part - odd_part)):
                            high, low = split(value)
                            at = slice(j * side + h * half + q, j * side + h * half + q + CHUNK)
                            lo_at = comp * half
                            lhs[odd, at, lo_at : lo_at + half] = high
                            lhs[odd, at, side + lo_at : side + lo_at + half] = low
                            lhs[odd, at, 2 * side + lo_at : 2 * side + lo_at + half] = high

        for odd in (0, 1):
            mid[odd] = dot(lhs[odd], lanes[2 * odd + 1])

        for j, slot in enumerate(slots):
            used = slot < count
            for h in (0, 1):
                for q in range(0, half, CHUNK):
                    at = slice(j * side + h * half + q, j * side + h * half + q + CHUNK)
                    even_part, odd_part = mid[0, at], mid[1, at]
                    for l, value in ((0, even_part + odd_part), (1, even_part - odd_part)):
                        v_re, v_im = value[:, :half], value[:, half:]
                        spot = (slice(h * half + q, h * half + q + CHUNK), slice(l * half, l * half + half))
                        p_re = rolled[(slot, 0) + spot]
                        p_im = rolled[(slot, 1) + spot]
                        cut = slice(q, q + CHUNK)
                        terms[slot, h, l, 0, cut] = jnp.where(used, p_re * v_re + p_im * v_im, 0.0)
                        terms[slot, h, l, 1, cut] = jnp.where(used, p_re * v_im - p_im * v_re, 0.0)
        return carry

    lax.fori_loop(0, (count + 1) // 2, visit, 0)

    norm = jnp.zeros((8, half), F32)
    for rz in (0, 1):
        for rk, out in ((0, own_out[rz]), (1, far_out[rz])):
            h = (rz ^ par_r) if rk else (rz ^ 1 ^ par_r)
            for cz in (0, 1):
                for ck in (0, 1):
                    l = (cz ^ par_c) if ck else (cz ^ 1 ^ par_c)
                    col_masks, row_marks = [], []
                    for slot in range(cap):
                        row_sign, row_from, col_sign, col_from = marks(slot)
                        own = (col_iota + l * half) * col_sign >= col_from
                        col_masks.append(jnp.logical_not(own) if ck else own)
                        row_marks.append((row_sign, row_from))
                    for q in range(0, half, CHUNK):
                        cut = slice(q, q + CHUNK)
                        acc = [None, None]
                        if rk == 0 and ck == 0:
                            for comp in (0, 1):
                                value = field[rz, cz, 0, comp, cut]
                                acc[comp] = RIDGE * value
                                sq = value * value
                                for e in range(0, CHUNK, 8):
                                    norm = norm + sq[e : e + 8]
                        for slot in range(cap):
                            row_sign, row_from = row_marks[slot]
                            spots = (row_iota + (h * half + q)) * row_sign
                            mask = (spots < row_from) if rk else (spots >= row_from)
                            mask = jnp.logical_and(mask, col_masks[slot])
                            for comp in (0, 1):
                                value = jnp.where(mask, terms[slot, h, l, comp, cut], 0.0)
                                acc[comp] = value if acc[comp] is None else acc[comp] + value
                        for comp in (0, 1):
                            out[cz, ck, comp, cut] = acc[comp]
    partial[0] = norm
    partial[1] += RIDGE * norm


def final_kernel(side, stage, *refs):
    half = side // 2
    sums = refs[: 2 * stage]
    refs = refs[2 * stage :]
    fields = refs[:stage]
    along_old = refs[stage]
    mine = refs[stage + 1 : stage + 5]
    theirs = refs[stage + 5 : stage + 9]
    solved, left = refs[stage + 9 :]
    par_r, par_c = parities()
    alphas, ratios = coefficients(stage, sums)
    for rz in (0, 1):
        for cz in (0, 1):
            for comp in (0, 1):
                for q in range(0, half, 2 * CHUNK):
                    cut = slice(q, q + 2 * CHUNK)
                    image = mine[2 * rz + cz][0, comp, cut] + theirs[2 * rz + cz][comp, cut]
                    value = image + ratios[-1] * along_old[rz, cz, 0, comp, cut]
                    residual = fields[-1][rz, cz, 0, comp, cut]
                    direction = fields[0][rz, cz, 0, comp, cut]
                    answer = alphas[0] * direction
                    for k in range(1, stage):
                        direction = fields[k][rz, cz, 0, comp, cut] + ratios[k] * direction
                        answer = answer + alphas[k] * direction
                    residual = residual - alphas[-1] * value
                    at = pl.ds(pl.multiple_of((rz ^ 1 ^ par_r) * half + q, 2 * CHUNK), 2 * CHUNK)
                    for right in (0, 1):
                        @pl.when((cz ^ 1 ^ par_c) == right)
                        def _():
                            solved[comp, at, right * half : right * half + half] = answer
                            left[comp, at, right * half : right * half + half] = residual


def call(kernel, outs, args, limit, scratch=()):
    return pl.pallas_call(
        kernel,
        out_shape=tuple(outs),
        in_specs=[SMEM if a.dtype == jnp.int32 else VMEM for a in args],
        out_specs=tuple([VMEM] * len(outs)),
        scratch_shapes=list(scratch),
        compiler_params=pltpu.CompilerParams(vmem_limit_bytes=limit * 2**20),
    )(*args)


def stages():
    out = []
    for axis in ("row", "col"):
        step = 1
        while step < lax.axis_size(axis):
            out.append((axis, step))
            step *= 2
    return out


class Running:
    def __init__(self, value):
        self.value, self.left = value, stages()

    def send(self):
        if not self.left:
            return jnp.zeros_like(self.value)
        axis, step = self.left.pop(0)
        count = lax.axis_size(axis)
        return lax.ppermute(self.value, axis, [(i, i ^ step) for i in range(count)])

    def finish(self):
        got = self.send()
        while self.left:
            self.value = self.value + got
            got = self.send()
        return [self.value, got]


def local(right_side, probe, detector_weights, offsets, counts):
    side = probe.shape[1]
    half = side // 2
    cap = offsets.shape[2]
    info = jnp.concatenate([counts.reshape(-1), offsets.reshape(-1)]).astype(jnp.int32)
    mats = jnp.asarray(tables(side))

    def shape(*dims, dtype=F32):
        return jax.ShapeDtypeStruct(dims, dtype)

    zone = shape(2, 2, half, half)
    strip = shape(2, 2, 2, half, half)
    whole = shape(4, 2, 2, 2, half, half)
    tiny = shape(2, 8, half)

    zones = call(functools.partial(zone_kernel, side), [zone, zone], [right_side], 4)
    beyond = [swap(zones[z], "col", z) for z in (0, 1)]
    rolled, weights, lanes, rows = call(
        functools.partial(prep_kernel, side, cap),
        [
            shape(cap, 2, side, side),
            shape(2, half, side),
            shape(4, 3 * side, side, dtype=BF16),
            shape(4, side, 3 * side, dtype=BF16),
        ],
        [info, probe, detector_weights, mats],
        8,
        [pltpu.VMEM((2, side, half), F32)],
    )
    near = call(first_kernel, [strip, strip], [*zones, *beyond], 4)
    far = [swap(near[z], "row", z) for z in (0, 1)]

    sums, fields = [], []
    field = along = None
    for stage in range(ITERS):
        args = [info, rolled, weights, lanes, rows, *sums, *near, *far]
        outs = [whole]
        if stage >= 1:
            args.append(field)
            outs.append(whole)
        if stage >= 2:
            args.append(along)
        got = call(
            functools.partial(apply_kernel, side, cap, stage),
            outs + [strip] * 4 + [tiny],
            args,
            16,
            [
                pltpu.VMEM((2, 2 * side, 3 * side), BF16),
                pltpu.VMEM((2, 2 * side, side), F32),
                pltpu.VMEM((2, 3 * side, 2 * side), BF16),
                pltpu.VMEM((2, side, 2 * side), F32),
                pltpu.VMEM((cap, 2, 2, 2, half, half), F32),
            ],
        )
        field, along = got[0], got[1] if stage >= 1 else None
        fields.append(field)
        own, sent, run = got[-5:-3], got[-3:-1], Running(got[-1])
        last = stage + 1 == ITERS
        from_b = swap(sent[1], "row", 1)
        from_a = swap(sent[0], "row", 0)
        part = shape(2, 2, half, half)
        *mine_a, run.value = call(
            reduce_kernel, [part, part, tiny], [own[0], from_a, run.value, run.send()], 4
        )
        if last:
            got_a = [swap(mine_a[cz][1], "col", cz) for cz in (0, 1)]
            (run.value,) = call(add_kernel, [tiny], [run.value, run.send()], 4)
        else:
            got_a = [swap(mine_a[cz], "col", cz) for cz in (0, 1)]
        *mine_b, run.value = call(
            reduce_kernel, [part, part, tiny], [own[1], from_b, run.value, run.send()], 4
        )
        if last:
            got_b = [swap(mine_b[cz][1], "col", cz) for cz in (0, 1)]
            sums = sums + run.finish()
            break
        got_b = [swap(mine_b[cz], "col", cz) for cz in (0, 1)]
        near_a, run.value = call(
            merge_kernel, [strip, tiny], [*mine_a, *got_a, run.value, run.send()], 4
        )
        far_a = swap(near_a, "row", 0)
        near_b, run.value = call(
            merge_kernel, [strip, tiny], [*mine_b, *got_b, run.value, run.send()], 4
        )
        far_b = swap(near_b, "row", 1)
        sums = sums + run.finish()
        near, far = (near_a, near_b), (far_a, far_b)

    out = shape(*right_side.shape)
    return call(
        functools.partial(final_kernel, side, ITERS),
        [out, out],
        [*sums, *fields, along, *mine_a, *mine_b, *got_a, *got_b],
        8,
    )


def solution(mesh):
    placed = (P(None, "row", "col"), P(), P(), P("row", "col", None, None), P("row", "col"))
    return jax.shard_map(
        local,
        mesh=mesh,
        in_specs=placed,
        out_specs=(P(None, "row", "col"), P(None, "row", "col")),
        check_vma=False,
    )
```
